32 devices in a mesh: dp: 16 (over z, x, core), tensor: 2 (over y).
Axes of the slice: x: 2, y: 2, z: 4, core: 2. Of those that a mesh axis runs over, the one named last changes fastest.
Arguments:
- tokens: bfloat16 [16384, 1024], P(('dp', 'tensor')), may hold values from -6 to 6
- seg_ids: int32 [16384], P('dp'), may hold values from 0 to 39, never falling along the last dimension, each value on 1 to 800 neighbouring positions
- forget: float32 [8, 16384], P('tensor', 'dp'), may hold values from 0.0002 to 0.8
- gate_logit: float32 [8, 16384], P('tensor', 'dp'), may hold values from -6 to 6
- d_out: float32 [16384, 1024], P(('dp', 'tensor')), may hold values from -6 to 6
- inward: float32 [1024, 3072], P('dp', 'tensor'), may hold values from -0.1875 to 0.1875
- outward: float32 [1024, 1024], P('tensor', 'dp'), may hold values from -0.5 to 0.5
- gateup: float32 [2, 1024, 2816], P(None, 'dp', 'tensor'), may hold values from -0.1875 to 0.1875
- downward: float32 [2816, 1024], P('tensor', 'dp'), may hold values from -0.109375 to 0.109375
- gains: float32 [2, 1024], replicated, may hold values from 0.5 to 1.5
- persist: float32 [16, 2048], replicated, may hold values from -6 to 6
- momentum_inward: float32 [1024, 3072], P('dp', 'tensor'), may hold values from -160 to 160
- momentum_outward: float32 [1024, 1024], P('tensor', 'dp'), may hold values from -160 to 160
- momentum_gateup: float32 [2, 1024, 2816], P(None, 'dp', 'tensor'), may hold values from -384 to 384
- momentum_downward: float32 [2816, 1024], P('tensor', 'dp'), may hold values from -256 to 256
- momentum_gains: float32 [2, 1024], replicated, may hold values from -768 to 768
- momentum_persist: float32 [16, 2048], replicated, may hold values from -80 to 80
- average_inward: float32 [1024, 3072], P('dp', 'tensor'), may hold values from -0.1875 to 0.1875
- average_outward: float32 [1024, 1024], P('tensor', 'dp'), may hold values from -0.5 to 0.5
- average_gateup: float32 [2, 1024, 2816], P(None, 'dp', 'tensor'), may hold values from -0.1875 to 0.1875
- average_downward: float32 [2816, 1024], P('tensor', 'dp'), may hold values from -0.109375 to 0.109375
- average_gains: float32 [2, 1024], replicated, may hold values from 0.5 to 1.5
- average_persist: float32 [16, 2048], replicated, may hold values from -6 to 6
Outputs:
- mixed: float32 [16384, 1024], P(('dp', 'tensor'))
- tokens_grad: float32 [16384, 1024], P(('dp', 'tensor'))
- grad_inward: float32 [1024, 3072], P('dp', 'tensor')
- next_inward: float32 [1024, 3072], P('dp', 'tensor')
- moment_inward: float32 [1024, 3072], P('dp', 'tensor')
- mean_inward: float32 [1024, 3072], P('dp', 'tensor')
- copy_inward: bfloat16 [1024, 3072], P('dp', 'tensor')
- grad_outward: float32 [1024, 1024], P('tensor', 'dp')
- next_outward: float32 [1024, 1024], P('tensor', 'dp')
- moment_outward: float32 [1024, 1024], P('tensor', 'dp')
- mean_outward: float32 [1024, 1024], P('tensor', 'dp')
- copy_outward: bfloat16 [1024, 1024], P('tensor', 'dp')
- grad_gateup: float32 [2, 1024, 2816], P(None, 'dp', 'tensor')
- next_gateup: float32 [2, 1024, 2816], P(None, 'dp', 'tensor')
- moment_gateup: float32 [2, 1024, 2816], P(None, 'dp', 'tensor')
- mean_gateup: float32 [2, 1024, 2816], P(None, 'dp', 'tensor')
- copy_gateup: bfloat16 [2, 1024, 2816], P(None, 'dp', 'tensor')
- grad_downward: float32 [2816, 1024], P('tensor', 'dp')
- next_downward: float32 [2816, 1024], P('tensor', 'dp')
- moment_downward: float32 [2816, 1024], P('tensor', 'dp')
- mean_downward: float32 [2816, 1024], P('tensor', 'dp')
- copy_downward: bfloat16 [2816, 1024], P('tensor', 'dp')
- grad_gains: float32 [2, 1024], replicated
- next_gains: float32 [2, 1024], replicated
- moment_gains: float32 [2, 1024], replicated
- mean_gains: float32 [2, 1024], replicated
- copy_gains: bfloat16 [2, 1024], replicated
- grad_persist: float32 [16, 2048], replicated
- next_persist: float32 [16, 2048], replicated
- moment_persist: float32 [16, 2048], replicated
- mean_persist: float32 [16, 2048], replicated
- copy_persist: bfloat16 [16, 2048], replicated
The draws below stay inside these ranges and needn't reach their ends.
Inputs may be any that keep to these rules, and one draw needn't show every extreme that they name: `seg_ids`: ids never fall along the tokens; each document holds 1 to 800 tokens, and some document exactly 800.
All inputs are finite; a program needn't handle non-finite values.
Results may differ from the reference program's by a relative error of at most 0.017.
Values may be sent and summed in bfloat16 or wider, within the bound.
A program may use at most 256 MiB of HBM per device.

```python
import math
import jax
import jax.numpy as jnp
import numpy as np
from jax import lax

D = 1024
ATTENDER_NUMBER = 8
FF = 2816
SEQ_LEN = 1024
SPAN = 64
PERSIST = 16
DOC_MOST = 800
WORD_SUM_ALL = 16384
DOCS = 40


def draw_forget(key, part):
    key_base = jax.random.fold_in(key, 11)
    key_rough = jax.random.fold_in(key, 12)
    key_where = jax.random.fold_in(key, 13)
    lookup_dimension = jax.random.fold_in(key, 14)
    lower, upper = (math.log(0.0005), math.log(0.04))
    starting_quantity = jnp.exp(jax.random.uniform(key_base, (ATTENDER_NUMBER, 1), jnp.float32, lower, upper))
    approximate_guess = jax.random.uniform(key_rough, (ATTENDER_NUMBER, WORD_SUM_ALL), jnp.float32, 0.5, 2.0)
    location_indices = (jax.random.randint(key_where, (ATTENDER_NUMBER, WORD_SUM_ALL), 0, 256) == 0).astype(jnp.float32)
    episode_span_size = location_indices * jax.random.uniform(lookup_dimension, (ATTENDER_NUMBER, WORD_SUM_ALL), jnp.float32, 0.2, 0.7)
    return jnp.clip(starting_quantity * approximate_guess + episode_span_size, 0.0002, 0.8)


def block_levels(rng, extent, cuts, low, largest):
    def one(dim, blocks):
        steps = jax.random.uniform(jax.random.fold_in(jax.random.fold_in(rng, 6), dim), (blocks,), jnp.float32, low / len(cuts), largest / len(cuts))
        return jnp.repeat(jnp.exp(steps), extent[dim] // blocks).reshape((-1,) + (1,) * (len(extent) - dim - 1))

    level = one(*cuts[0])
    for cut in cuts[1:]:
        level = level * one(*cut)
    return level


def split_up(count, total, most, lean):
    weights = [(1 << 20) // math.isqrt(grade ** lean) + 1 for grade in range(2, count + 1)]
    spare, given = total - most - (count - 1), [1] * (count - 1)
    while spare > 0:
        candidates = [i for i in range(count - 1) if given[i] < most]
        mass, left = sum([weights[i] for i in candidates]), spare
        for i in candidates:
            addition = min(most - given[i], max(1, left * weights[i] // mass), spare)
            given[i] = given[i] + addition
            spare = spare - addition
    return np.array([most] + given)


def ragged(stream_key, amount, total, reach, slope):
    if amount == 2:
        one = jax.random.randint(stream_key, (), max(1, total - reach), min(reach, total - 1) + 1)
        return jnp.stack([one, total - one])
    sizes = jnp.asarray(split_up(amount, total, reach, slope), jnp.int32)
    pairs = (amount - 1) // 2
    source_of, sink = sizes[1:1 + 2 * pairs:2], sizes[2:2 + 2 * pairs:2]
    margin = jnp.minimum(source_of - 1, reach - sink)
    moved = jax.random.randint(jax.random.fold_in(stream_key, 1), (pairs,), 0, 1 << 20) % (margin + 1)
    sizes = sizes.at[1:1 + 2 * pairs:2].set(source_of - moved).at[2:2 + 2 * pairs:2].set(sink + moved)
    return sizes[jax.random.permutation(jax.random.fold_in(stream_key, 2), amount)]


def noise(key, shape, scale, most, cuts=(), held_as=jnp.bfloat16):
    values = scale * jax.random.normal(key, shape, jnp.float32)
    if cuts:
        values = values * block_levels(key, shape, cuts, -0.22, 0.18)
    return jnp.clip(values, -most, most).astype(held_as)


def setup_inputs(seed: int = 0) -> dict:
    keys = jax.random.split(jax.random.key(seed), 24)
    tokens = noise(keys[0], (WORD_SUM_ALL, D), 1.0, 6.0, ((0, 32),))
    seg_ids = jnp.searchsorted(jnp.cumsum(ragged(keys[1], DOCS, WORD_SUM_ALL, DOC_MOST, 0)), jnp.arange(WORD_SUM_ALL), side="right").astype(jnp.int32)
    forget = draw_forget(jax.random.fold_in(keys[23], 71), 0)
    gate_logit = noise(keys[3], (ATTENDER_NUMBER, WORD_SUM_ALL), 1.5, 6.0, ((0, 2), (1, 16)), jnp.float32)
    d_out = noise(keys[4], (WORD_SUM_ALL, D), 1.0, 6.0, ((0, 32),), jnp.float32)
    inward = noise(keys[5], (D, 3 * D), D ** -0.5, 0.1875, ((0, 16), (1, 2)), jnp.float32)
    outward = noise(keys[6], (D, D), (D // 8) ** -0.5, 0.5, ((0, 2), (1, 16)), jnp.float32)
    gateup = noise(keys[7], (2, D, FF), D ** -0.5, 0.1875, ((1, 16), (2, 2)), jnp.float32)
    downward = noise(keys[8], (FF, D), FF ** -0.5, 0.109375, ((0, 2), (1, 16)), jnp.float32)
    gains = jnp.clip(1.0 + 0.1 * jax.random.normal(keys[9], (2, D), jnp.float32), 0.5, 1.5)
    persist = noise(keys[10], (PERSIST, 2 * D), 1.0, 6.0, (), jnp.float32)
    momentum_inward = noise(keys[11], (D, 3 * D), ((WORD_SUM_ALL // 25) ** 0.5), 160.0, ((0, 16), (1, 2)), jnp.float32)
    momentum_outward = noise(keys[12], (D, D), ((WORD_SUM_ALL // 25) ** 0.5), 160.0, ((0, 2), (1, 16)), jnp.float32)
    momentum_gateup = noise(keys[13], (2, D, FF), ((WORD_SUM_ALL // 4) ** 0.5), 384.0, ((1, 16), (2, 2)), jnp.float32)
    momentum_downward = noise(keys[14], (FF, D), ((WORD_SUM_ALL // 9) ** 0.5), 256.0, ((0, 2), (1, 16)), jnp.float32)
    momentum_gains = noise(keys[15], (2, D), (WORD_SUM_ALL ** 0.5), 768.0, (), jnp.float32)
    momentum_persist = noise(keys[16], (PERSIST, 2 * D), ((WORD_SUM_ALL // 100) ** 0.5), 80.0, (), jnp.float32)
    average_inward = noise(keys[17], (D, 3 * D), D ** -0.5, 0.1875, ((0, 16), (1, 2)), jnp.float32)
    average_outward = noise(keys[18], (D, D), (D // 8) ** -0.5, 0.5, ((0, 2), (1, 16)), jnp.float32)
    average_gateup = noise(keys[19], (2, D, FF), D ** -0.5, 0.1875, ((1, 16), (2, 2)), jnp.float32)
    average_downward = noise(keys[20], (FF, D), FF ** -0.5, 0.109375, ((0, 2), (1, 16)), jnp.float32)
    average_gains = jnp.clip(1.0 + 0.1 * jax.random.normal(keys[21], (2, D), jnp.float32), 0.5, 1.5)
    average_persist = noise(keys[22], (PERSIST, 2 * D), 1.0, 6.0, (), jnp.float32)
    return dict(tokens=tokens, seg_ids=seg_ids, forget=forget, gate_logit=gate_logit, d_out=d_out, inward=inward, outward=outward, gateup=gateup, downward=downward, gains=gains, persist=persist, momentum_inward=momentum_inward, momentum_outward=momentum_outward, momentum_gateup=momentum_gateup, momentum_downward=momentum_downward, momentum_gains=momentum_gains, momentum_persist=momentum_persist, average_inward=average_inward, average_outward=average_outward, average_gateup=average_gateup, average_downward=average_downward, average_gains=average_gains, average_persist=average_persist)


@jax.custom_vjp
def low(v):
    return lax.optimization_barrier(v.astype(jnp.bfloat16)).astype(jnp.float32)

@jax.custom_vjp
def low_back(v):
    return v

def low_keep(v):
    return (low(v), None)

def low_pass(kept, grad):
    return (grad,)

def back_keep(v):
    return (v, None)

def back_low(kept, grad):
    return (low(grad),)
low.defvjp(low_keep, low_pass)
low_back.defvjp(back_keep, back_low)
EPS = 1e-06
HIGH = lax.Precision.HIGHEST
LEARN = 0.0003
LEARN_PERSIST = 0.012
MOMENT_RATE = 0.5
AVERAGE_RATE = 0.5

def unit_rows(value):
    return value * lax.rsqrt(lax.optimization_barrier(jnp.sum(value * value, -1, keepdims=True)) + EPS)

def memory_block(carry, block):
    state, last_seg = carry
    query_n, key_n, value, seg, rate = block
    size = seg.shape[0]
    level = jnp.cumsum(rate, axis=-1)
    place = jnp.arange(size)
    allowed = (seg[:, None] == seg[None, :]) & (place[None, :] <= place[:, None])
    gap = jnp.where(allowed[None], level[:, :, None] - level[:, None, :], 60.0)
    weights = jnp.exp(-gap) * allowed[None].astype(jnp.float32)
    dots = jnp.einsum('thd,shd->hts', query_n, key_n, precision=HIGH)
    inner = jnp.einsum('hts,shd->thd', weights * dots, value, precision=HIGH)
    keep = (seg == last_seg).astype(jnp.float32)
    factor = jnp.exp(-level).T * keep[:, None]
    carried = jnp.einsum('thd,hde->the', query_n, state, precision=HIGH) * factor[:, :, None]
    tail = jnp.exp(-(level[:, -1:] - level)) * (seg == seg[-1]).astype(jnp.float32)[None, :]
    fresh = jnp.einsum('shd,she,hs->hde', key_n, value, tail, precision=HIGH)
    hold = jnp.exp(-level[:, -1]) * (seg[-1] == last_seg).astype(jnp.float32)
    state = state * hold[:, None, None] + fresh
    return ((state, seg[-1]), inner + carried)

def sequence_core(query, key_in, value, persist_k, persist_v, seg, rate, gate):
    length, heads, width = query.shape
    scale = width ** (-0.5)
    place = jnp.arange(length)
    allowed = (seg[:, None] == seg[None, :]) & (place[None, :] <= place[:, None])
    own = jnp.einsum('thd,shd->hts', query, key_in, precision=HIGH) * scale
    own = jnp.where(allowed[None], own, -1e+30)
    fixed = jnp.einsum('thd,phd->htp', query, persist_k, precision=HIGH) * scale
    probs = jax.nn.softmax(jnp.concatenate([own, fixed], -1), axis=-1)
    attended = jnp.einsum('hts,shd->thd', probs[:, :, :length], value, precision=HIGH)
    attended = attended + jnp.einsum('htp,phd->thd', probs[:, :, length:], persist_v, precision=HIGH)
    blocks = length // SPAN
    query_n = unit_rows(query).reshape(blocks, SPAN, heads, width)
    key_n = unit_rows(key_in).reshape(blocks, SPAN, heads, width)
    value_b = value.reshape(blocks, SPAN, heads, width)
    seg_b = seg.reshape(blocks, SPAN)
    rate_b = rate.reshape(heads, blocks, SPAN).transpose(1, 0, 2)
    start = (jnp.zeros((heads, width, width), jnp.float32), jnp.array(-1, jnp.int32))
    carry_end, recalled = lax.scan(jax.checkpoint(memory_block), start, (query_n, key_n, value_b, seg_b, rate_b))
    recalled = recalled.reshape(length, heads, width)
    mixed = attended + jax.nn.sigmoid(gate).T[:, :, None] * recalled
    return mixed.reshape(length, heads * width)

def group_core(qkv, persist_cols, seg, rate, gate):
    total = qkv.shape[0]
    heads = rate.shape[0]
    width = qkv.shape[1] // (3 * heads)
    parts = qkv.reshape(total, heads, 3, width)
    pairs = persist_cols.reshape(persist_cols.shape[0], heads, 2, width)
    persist_k = pairs[:, :, 0]
    persist_v = pairs[:, :, 1]
    count = total // SEQ_LEN

    def one_sequence(item):
        query, key_in, value, seq_seg, seq_rate, seq_gate = item
        return sequence_core(query, key_in, value, persist_k, persist_v, seq_seg, seq_rate, seq_gate)

    def split_rows(array):
        return array.reshape((count, SEQ_LEN) + array.shape[1:])

    def split_heads(array):
        return array.reshape(heads, count, SEQ_LEN).transpose(1, 0, 2)
    result = lax.map(jax.checkpoint(one_sequence), (split_rows(parts[:, :, 0]), split_rows(parts[:, :, 1]), split_rows(parts[:, :, 2]), split_rows(seg), split_heads(rate), split_heads(gate)))
    return result.reshape(total, heads * width)

def matmul(left, right):
    return jnp.dot(left, right, precision=HIGH, preferred_element_type=jnp.float32)

def advance(weight, moment, average, grad, step_rate=LEARN):
    moment_new = MOMENT_RATE * moment + grad
    weight_new = weight - step_rate * (grad + MOMENT_RATE * moment_new)
    average_new = AVERAGE_RATE * average + (1.0 - AVERAGE_RATE) * weight_new
    return (grad, weight_new, moment_new, average_new, weight_new.astype(jnp.bfloat16))

def reference(tokens, seg_ids, forget, gate_logit, d_out, inward, outward, gateup, downward, gains, persist, momentum_inward, momentum_outward, momentum_gateup, momentum_downward, momentum_gains, momentum_persist, average_inward, average_outward, average_gateup, average_downward, average_gains, average_persist):

    def forward(x, w_in, w_out, w_gu, w_down, gain_rows, persist_rows):
        rms1 = lax.rsqrt(lax.optimization_barrier(jnp.mean(x * x, -1, keepdims=True)) + EPS)
        normed1 = low(x * rms1 * gain_rows[0])
        qkv = low(low_back(matmul(normed1, low(w_in))))
        heads = low(group_core(qkv, persist_rows, seg_ids, forget, gate_logit))
        branch = low_back(matmul(heads, low(w_out)))
        middle = x + branch
        rms2 = lax.rsqrt(lax.optimization_barrier(jnp.mean(middle * middle, -1, keepdims=True)) + EPS)
        normed2 = low(middle * rms2 * gain_rows[1])
        gate_pre = low_back(matmul(normed2, low(w_gu[0])))
        up_pre = low_back(matmul(normed2, low(w_gu[1])))
        hidden = low(jax.nn.silu(gate_pre) * up_pre)
        return middle + low_back(matmul(hidden, low(w_down)))
    x = tokens.astype(jnp.float32)
    mixed, backward = jax.vjp(forward, x, inward, outward, gateup, downward, gains, persist)
    tokens_grad, g_in, g_out, g_gu, g_down, g_gains, g_persist = backward(d_out)
    a1, a2, a3, a4, a5 = advance(inward, momentum_inward, average_inward, g_in)
    b1, b2, b3, b4, b5 = advance(outward, momentum_outward, average_outward, g_out)
    c1, c2, c3, c4, c5 = advance(gateup, momentum_gateup, average_gateup, g_gu)
    e1, e2, e3, e4, e5 = advance(downward, momentum_downward, average_downward, g_down)
    f1, f2, f3, f4, f5 = advance(gains, momentum_gains, average_gains, g_gains)
    h1, h2, h3, h4, h5 = advance(persist, momentum_persist, average_persist, g_persist, LEARN_PERSIST)
    return (mixed, tokens_grad, a1, a2, a3, a4, a5, b1, b2, b3, b4, b5, c1, c2, c3, c4, c5, e1, e2, e3, e4, e5, f1, f2, f3, f4, f5, h1, h2, h3, h4, h5)
```

```python
import functools
import jax
import jax.numpy as jnp
from jax import lax
from jax.experimental import pallas as pl
from jax.experimental.pallas import tpu as pltpu

EPS = 1e-06
LOG2E = 1.4426950408889634
HIDE = -1e30
TILE = 256
FIXED = 16


def flip(a):
    return a.astype(jnp.float32).T


def running_sum(row):
    lane = lax.broadcasted_iota(jnp.int32, row.shape, 1)
    step = 1
    while step < row.shape[1]:
        row = row + jnp.where(lane >= step, pltpu.roll(row, step, 1), 0.0)
        step *= 2
    return row


def level_terms(q_t, keys, rate, gate):
    length = q_t.shape[1]
    level = running_sum(rate)
    log_sig = jnp.minimum(gate, 0.0) - jnp.log(1.0 + jnp.exp(-jnp.abs(gate)))
    norm_q = jnp.sum(q_t * q_t, 0, keepdims=True) + EPS
    row = level - log_sig + 0.5 * jnp.log(norm_q)
    wide = keys.astype(jnp.float32)
    norm_k = jnp.sum(wide * wide, 1, keepdims=True) + EPS
    column = jnp.broadcast_to(level, (128, length)).T - 0.5 * jnp.log(norm_k)
    return row * LOG2E, column * LOG2E, norm_q, norm_k


def tile_terms(scores, seg_c, seg_r, column, row, diagonal):
    mask = seg_c == seg_r
    if diagonal:
        down = lax.broadcasted_iota(jnp.int32, scores.shape, 0)
        across = lax.broadcasted_iota(jnp.int32, scores.shape, 1)
        mask = mask & (down <= across)
    decay = jnp.exp2(jnp.where(mask, column - row, HIDE))
    return jnp.where(mask, scores, HIDE), decay


def dot32(a, b):
    return jnp.dot(a, b, preferred_element_type=jnp.float32)


def ordered(ref, turn, columns):
    rows = ref.shape[0] // 2
    first = pl.multiple_of(turn * rows, rows)
    last = pl.multiple_of((1 - turn) * rows, rows)
    return jnp.concatenate([ref[pl.ds(first, rows), columns], ref[pl.ds(last, rows), columns]], 0)


def stored(start, turn, length):
    return pl.ds(pl.multiple_of(lax.rem(start + turn * (length // 2), length), TILE), TILE)


def core_fwd_kernel(turn_ref, qkv_ref, fixed_ref, rate_ref, gate_ref, segr_ref, segc_ref, heads_ref, att_ref, lse_ref, col_scr):
    half = jnp.bfloat16
    length = qkv_ref.shape[0]
    scale = 128 ** (-0.5) * LOG2E
    turn = turn_ref[0]
    keys = ordered(qkv_ref, turn, slice(128, 256))
    q_t = flip(ordered(qkv_ref, turn, slice(0, 128)))
    v_t = flip(ordered(qkv_ref, turn, slice(256, 384))).astype(half)
    row, column, _, _ = level_terms(q_t, keys, rate_ref[0], gate_ref[0])
    col_scr[...] = column
    q_t = q_t.astype(half)
    fixed_k = fixed_ref[:, 0:128].astype(half)
    fixed_vt = fixed_ref[:, 128:256].T.astype(half)
    for j in range(length // TILE):
        cols = slice(j * TILE, (j + 1) * TILE)
        q_j = q_t[:, cols]
        seg_r = segr_ref[:, cols]
        row_j = row[:, cols]
        s_fix = dot32(fixed_k, q_j)
        top = jnp.max(s_fix, 0, keepdims=True)
        kept = []
        carry = jnp.zeros((128, TILE), jnp.float32)
        for i in range(j + 1):
            rows = slice(i * TILE, (i + 1) * TILE)
            scores = dot32(keys[rows], q_j)
            wide = jnp.concatenate([col_scr[rows, :]] * (TILE // 128), 1)
            hidden, decay = tile_terms(scores, segc_ref[rows, :], seg_r, wide, row_j, i == j)
            top = jnp.maximum(top, jnp.max(hidden, 0, keepdims=True))
            carry = carry + dot32(v_t[:, rows], (scores * decay).astype(half))
            kept.append(hidden)
        top = top * scale
        p_fix = jnp.exp2(s_fix * scale - top)
        total = jnp.sum(p_fix, 0, keepdims=True)
        acc = dot32(fixed_vt, p_fix.astype(half))
        for i in range(j + 1):
            rows = slice(i * TILE, (i + 1) * TILE)
            probs = jnp.exp2(kept[i] * scale - top)
            total = total + jnp.sum(probs, 0, keepdims=True)
            acc = acc + dot32(v_t[:, rows], probs.astype(half))
        att = acc / total
        att_ref[0, :, cols] = att
        lse_ref[0, :, cols] = top + jnp.log(total) * LOG2E
        heads_ref[stored(j * TILE, turn, length), :] = (att + carry).T.astype(half)


def core_bwd_kernel(turn_ref, qkv_ref, fixed_ref, rate_ref, gate_ref, segr_ref, segc_ref, grad_ref, att_ref, lse_ref,
                    dqkv_ref, dfix_ref, col_scr, dk_scr, dv_scr, sum_scr):
    half = jnp.bfloat16
    length = qkv_ref.shape[0]
    plain = 128 ** (-0.5)
    scale = plain * LOG2E
    turn = turn_ref[0]
    keys = ordered(qkv_ref, turn, slice(128, 256))
    values = ordered(qkv_ref, turn, slice(256, 384))
    q_t = flip(ordered(qkv_ref, turn, slice(0, 128)))
    k_t = flip(keys).astype(half)
    row, column, norm_q, norm_k = level_terms(q_t, keys, rate_ref[0], gate_ref[0])
    col_scr[...] = column
    dk_scr[...] = jnp.zeros_like(dk_scr)
    dv_scr[...] = jnp.zeros_like(dv_scr)
    sum_scr[...] = jnp.zeros_like(sum_scr)
    g_t = flip(ordered(grad_ref, turn, slice(0, 128)))
    fixed_k = fixed_ref[:, 0:128].astype(half)
    fixed_kt = fixed_ref[:, 0:128].T.astype(half)
    fixed_v = fixed_ref[:, 128:256].astype(half)
    dfix_k = jnp.zeros((FIXED, 128), jnp.float32)
    dfix_v = jnp.zeros((FIXED, 128), jnp.float32)
    for j in range(length // TILE):
        cols = slice(j * TILE, (j + 1) * TILE)
        qf_j = q_t[:, cols]
        q_j = qf_j.astype(half)
        gf_j = g_t[:, cols]
        g_j = gf_j.astype(half)
        place = stored(j * TILE, turn, length)
        q_rows = qkv_ref[place, 0:128]
        g_rows = grad_ref[place, :].astype(half)
        seg_r = segr_ref[:, cols]
        row_j = row[:, cols]
        lse = lse_ref[0, :, cols]
        delta = jnp.sum(gf_j * att_ref[0, :, cols], 0, keepdims=True)
        p_fix = jnp.exp2(dot32(fixed_k, q_j) * scale - lse)
        d_fix = p_fix * (dot32(fixed_v, g_j) - delta) * plain
        p_half = p_fix.astype(half)
        d_half = d_fix.astype(half)
        dfix_v = dfix_v + dot32(p_half, g_rows)
        dfix_k = dfix_k + dot32(d_half, q_rows)
        dq_t = dot32(fixed_kt, d_half)
        inner = jnp.zeros((1, TILE), jnp.float32)
        for i in range(j + 1):
            rows = slice(i * TILE, (i + 1) * TILE)
            scores = dot32(keys[rows], q_j)
            d_a = dot32(values[rows], g_j)
            wide = jnp.concatenate([col_scr[rows, :]] * (TILE // 128), 1)
            hidden, decay = tile_terms(scores, segc_ref[rows, :], seg_r, wide, row_j, i == j)
            probs = jnp.exp2(hidden * scale - lse)
            flow = d_a * decay
            both = flow * scores
            inner = inner + jnp.sum(both, 0, keepdims=True)
            sum_scr[rows, :] = sum_scr[rows, :] + sum(both[:, n * 128:(n + 1) * 128] for n in range(TILE // 128))
            mix = (probs + scores * decay).astype(half)
            d_s = (probs * (d_a - delta) * plain + flow).astype(half)
            dv_scr[rows, :] = dv_scr[rows, :] + dot32(mix, g_rows)
            dk_scr[rows, :] = dk_scr[rows, :] + dot32(d_s, q_rows)
            dq_t = dq_t + dot32(k_t[:, rows], d_s)
        dq_t = dq_t - qf_j * (inner / norm_q[:, cols])
        dqkv_ref[place, 0:128] = dq_t.T.astype(half)
    side = jnp.sum(sum_scr[...], 1, keepdims=True) / norm_k
    d_keys = (dk_scr[...] - keys.astype(jnp.float32) * side).astype(half)
    d_values = dv_scr[...].astype(half)
    for j in range(length // TILE):
        cols = slice(j * TILE, (j + 1) * TILE)
        place = stored(j * TILE, turn, length)
        dqkv_ref[place, 128:256] = d_keys[cols]
        dqkv_ref[place, 256:384] = d_values[cols]
    dfix_ref[0, :, 0:128] = dfix_k
    dfix_ref[0, :, 128:256] = dfix_v


def core_specs(length):
    return [
        pl.BlockSpec((length, 384), lambda b, h, t: (b, h)),
        pl.BlockSpec((FIXED, 256), lambda b, h, t: (0, h)),
        pl.BlockSpec((1, 1, length), lambda b, h, t: (h, 0, b)),
        pl.BlockSpec((1, 1, length), lambda b, h, t: (h, 0, b)),
        pl.BlockSpec((1, length), lambda b, h, t: (0, b)),
        pl.BlockSpec((length, 1), lambda b, h, t: (b, 0)),
    ]


def core_fwd(qkv, fixed, rate, gate, seg, length, turn):
    total, heads = qkv.shape[0], qkv.shape[1] // 384
    count = total // length
    args = (turn.reshape(1), qkv, fixed, rate[:, None], gate[:, None], seg[None], seg[:, None])
    return pl.pallas_call(
        core_fwd_kernel,
        grid_spec=pltpu.PrefetchScalarGridSpec(
            num_scalar_prefetch=1,
            grid=(count, heads),
            in_specs=core_specs(length),
            out_specs=[
            pl.BlockSpec((length, 128), lambda b, h, t: (b, h)),
            pl.BlockSpec((1, 128, length), lambda b, h, t: (h, 0, b)),
            pl.BlockSpec((1, 1, length), lambda b, h, t: (h, 0, b)),
            ],
            scratch_shapes=[pltpu.VMEM((length, 128), jnp.float32)],
        ),
        out_shape=[
            jax.ShapeDtypeStruct((total, heads * 128), jnp.bfloat16),
            jax.ShapeDtypeStruct((heads, 128, total), jnp.float32),
            jax.ShapeDtypeStruct((heads, 1, total), jnp.float32),
        ],
        name="core_fwd",
    )(*args)


def core_bwd(qkv, fixed, rate, gate, seg, grad, att, lse, length, turn):
    total, heads = qkv.shape[0], qkv.shape[1] // 384
    count = total // length
    args = (turn.reshape(1), qkv, fixed, rate[:, None], gate[:, None], seg[None], seg[:, None], grad, att, lse)
    dqkv, dfix = pl.pallas_call(
        core_bwd_kernel,
        grid_spec=pltpu.PrefetchScalarGridSpec(
            num_scalar_prefetch=1,
            grid=(count, heads),
            in_specs=core_specs(length) + [
            pl.BlockSpec((length, 128), lambda b, h, t: (b, h)),
            pl.BlockSpec((1, 128, length), lambda b, h, t: (h, 0, b)),
            pl.BlockSpec((1, 1, length), lambda b, h, t: (h, 0, b)),
        ],
        out_specs=[
            pl.BlockSpec((length, 384), lambda b, h, t: (b, h)),
            pl.BlockSpec((1, FIXED, 256), lambda b, h, t: (b, 0, h)),
            ],
            scratch_shapes=[pltpu.VMEM((length, 128), jnp.float32)] * 4,
        ),
        out_shape=[
            jax.ShapeDtypeStruct((total, heads * 384), jnp.bfloat16),
            jax.ShapeDtypeStruct((count, FIXED, heads * 256), jnp.float32),
        ],
        name="core_bwd",
    )(*args)
    return dqkv, jnp.sum(dfix, 0)


from jax.sharding import PartitionSpec as P

SEQ_LEN = 1024
LEARN = 0.0003
LEARN_PERSIST = 0.012
MOMENT_RATE = 0.5
AVERAGE_RATE = 0.5


def product(left, right):
    return jnp.dot(left, right, preferred_element_type=jnp.float32)


def product_nt(left, right):
    return lax.dot_general(left, right, (((1,), (1,)), ((), ())), preferred_element_type=jnp.float32)


def product_tn(left, right):
    return lax.dot_general(left, right, (((0,), (0,)), ((), ())), preferred_element_type=jnp.float32)


def inverse_rms(rows):
    return lax.rsqrt(jnp.mean(rows * rows, -1, keepdims=True) + EPS)


def norm_back(inputs, scale_rows, gain_row, grad):
    gain_grad = jnp.sum(grad * inputs * scale_rows, 0)
    scaled = grad * gain_row
    inner = jnp.mean(scaled * inputs, -1, keepdims=True)
    return (scale_rows * scaled - inputs * scale_rows**3 * inner, gain_grad)


def advance(weight, moment, average, grad, step_rate=LEARN):
    moment_new = MOMENT_RATE * moment + grad
    weight_new = weight - step_rate * (grad + MOMENT_RATE * moment_new)
    average_new = AVERAGE_RATE * average + (1.0 - AVERAGE_RATE) * weight_new
    return (grad, weight_new, moment_new, average_new, weight_new.astype(jnp.bfloat16))


def after(value, *done):
    return lax.optimization_barrier((value, *done))[0]


class Group:
    def __init__(self, size):
        self.size = size
        self.pair = size == 2

    def other(self, rows):
        return lax.ppermute(rows, "tensor", [(0, 1), (1, 0)])

    def gather(self, rows, *done):
        if self.pair:
            sent = self.other(after(rows, *done) if done else rows)
            return jnp.concatenate([rows, sent], 0), sent
        wide = lax.all_gather(rows, "tensor", axis=0, tiled=True)
        return wide, wide

    def scatter(self, make, *operands, done=()):
        if self.pair:
            mine = operands[0].shape[0] // 2
            away = make(*[a[mine:] for a in operands]).astype(jnp.bfloat16)
            sent = self.other(after(away, *done) if done else away)
            own = lax.optimization_barrier(make(*[a[:mine] for a in operands]))
            return own + sent.astype(jnp.float32), (own, away)
        part = make(*operands).astype(jnp.bfloat16)
        return lax.psum_scatter(part, "tensor", scatter_dimension=0, tiled=True).astype(jnp.float32), (part,)


def place_kernel(offsets_ref, *refs):
    pieces, full_ref, sems = refs[:-2], refs[-2], refs[-1]
    rows = full_ref.shape[0] // 16
    copies = []
    start = 0
    for n in range(0, len(pieces), 4):
        width = pieces[n].shape[1]
        for m in range(4):
            for k in range(4):
                at = pl.multiple_of(offsets_ref[4 * m + k], rows)
                copies.append(pltpu.make_async_copy(
                    pieces[n + m].at[pl.ds(k * rows, rows)],
                    full_ref.at[pl.ds(at, rows), pl.ds(start, width)],
                    sems.at[len(copies)],
                ))
                copies[-1].start()
        start += width
    for copy in copies:
        copy.wait()


def place(offsets, pieces):
    width = sum(piece.shape[1] for piece in pieces[::4])
    rows = 4 * pieces[0].shape[0]
    return pl.pallas_call(
        place_kernel,
        grid_spec=pltpu.PrefetchScalarGridSpec(
            num_scalar_prefetch=1,
            grid=(1,),
            in_specs=[pl.BlockSpec(memory_space=pl.ANY)] * len(pieces),
            out_specs=pl.BlockSpec((rows, width), lambda n, t: (0, 0), pipeline_mode=pl.Buffered(1)),
            scratch_shapes=[pltpu.SemaphoreType.DMA((4 * len(pieces),))],
        ),
        out_shape=jax.ShapeDtypeStruct((rows, width), jnp.bfloat16),
        name="place",
    )(offsets, *pieces)


class Ring:
    def __init__(self, size, pair):
        self.size = size
        self.cube = size == 16 and pair

    def swap(self, rows, bits):
        return lax.ppermute(rows, "dp", [(n, n ^ bits) for n in range(self.size)])

    def spots(self):
        me = lax.axis_index("dp")
        return me // 4, lax.rem(me // 2, 2), lax.rem(me, 2)

    def gather(self, shard, cuts, done):
        shard = shard.astype(jnp.bfloat16)
        if not self.cube:
            full = lax.all_gather(shard, "dp", axis=0, tiled=True)
            return full, full
        rows = shard.shape[0]
        z, x, core = self.spots()
        spots = [((z ^ k) * 4 + jnp.bitwise_xor(x, m % 2) * 2 + jnp.bitwise_xor(core, m // 2)) * rows
                 for m in range(4) for k in range(4)]
        pieces = []
        edges = [0, *cuts, shard.shape[1]]
        for low, high in zip(edges[:-1], edges[1:]):
            part = shard[:, low:high]
            if done is not None:
                part = after(part, done)
            line = [self.swap(part, 4 * k) for k in (1, 2, 3)]
            done = line[-1]
            here = jnp.concatenate([part, *line], 0)
            there = self.swap(here, 2)
            pieces += [here, there, self.swap(here, 1), self.swap(there, 1)]
        return place(jnp.stack(spots).astype(jnp.int32), pieces), done

    def scatter(self, grad, cuts=()):
        grad = grad.astype(jnp.bfloat16)
        if not self.cube:
            return lax.psum_scatter(grad, "dp", scatter_dimension=0, tiled=True).astype(jnp.float32)
        z, x, core = self.spots()
        rows = grad.shape[0] // 16
        pick = functools.partial(lax.dynamic_index_in_dim, keepdims=False)
        sums = []
        edges = [0, *cuts, grad.shape[1]]
        for low, high in zip(edges[:-1], edges[1:]):
            part = grad[:, low:high].reshape(4, 2, 2, rows, high - low)
            near = self.swap(pick(part, 1 - core, 2), 1)
            kept = pick(part, core, 2)

            def two(at):
                return pick(kept, at, 1).astype(jnp.float32) + pick(near, at, 1).astype(jnp.float32)

            across = self.swap(two(1 - x).astype(jnp.bfloat16), 2)
            four = two(x)

            def three(at):
                return pick(four, at, 0) + pick(across, at, 0).astype(jnp.float32)

            total = three(z)
            for k in (1, 2, 3):
                total = total + self.swap(three(z ^ k).astype(jnp.bfloat16), 4 * k).astype(jnp.float32)
            sums.append(total)
        return jnp.concatenate(sums, 1)

    def total(self, *values):
        if not self.cube:
            return lax.psum(values, "dp")
        for bits in (1, 2, 4, 8):
            values = [value + self.swap(value, bits) for value in values]
        return values


def shards(group, ring, tokens, seg_ids, forget, gate_logit, d_out, inward, outward, gateup, downward, gains, persist,
           momentum_inward, momentum_outward, momentum_gateup, momentum_downward, momentum_gains, momentum_persist,
           average_inward, average_outward, average_gateup, average_downward, average_gains, average_persist):
    half = jnp.bfloat16
    x = tokens.astype(jnp.float32)
    rms1 = inverse_rms(x)
    normed1 = (x * rms1 * gains[0]).astype(half)
    width = inward.shape[1]
    w_in, done = ring.gather(inward, (width // 2,), None)
    wide_one, one_done = group.gather(normed1)
    w_out, done = ring.gather(outward.T, (), done)
    w_gate, done = ring.gather(gateup[0], (), done)
    w_up, done = ring.gather(gateup[1], (), done)
    w_down, done = ring.gather(downward.T, (), done)
    cot, _ = group.gather(d_out.astype(half), one_done)
    head_cols = w_out.shape[1]
    place_at = lax.axis_index("tensor")
    start = place_at * (2 * head_cols)
    turn = place_at if group.pair else jnp.int32(0)
    persist_cols = lax.dynamic_slice_in_dim(persist, start, 2 * head_cols, 1)

    qkv = product(wide_one, w_in).astype(half)
    core = (qkv, persist_cols, forget, gate_logit, seg_ids)
    heads, att, lse = core_fwd(*core, SEQ_LEN, turn)
    branch, _ = group.scatter(lambda a: product_nt(a, w_out), heads)
    middle = x + branch
    rms2 = inverse_rms(middle)
    normed2 = (middle * rms2 * gains[1]).astype(half)
    wide_two, _ = group.gather(normed2)
    gate_pre = product(wide_two, w_gate)
    up_pre = product(wide_two, w_up)
    sigma = jax.nn.sigmoid(gate_pre)
    hidden = (gate_pre * sigma * up_pre).astype(half)
    d_hidden = product(cot, w_down)
    d_gate = (d_hidden * up_pre * sigma * (1.0 + gate_pre * (1.0 - sigma))).astype(half)
    d_up = (d_hidden * gate_pre * sigma).astype(half)
    dnormed2, _ = group.scatter(lambda a, b: product_nt(a, w_gate) + product_nt(b, w_up), d_gate, d_up)
    g_down = ring.scatter(product_tn(cot, hidden)).T
    g_gu = jnp.stack([ring.scatter(product_tn(wide_two, d_gate)), ring.scatter(product_tn(wide_two, d_up))])
    dmiddle_norm, gain_two = norm_back(middle, rms2, gains[1], dnormed2)
    dmiddle = d_out + dmiddle_norm
    attn_cot, cot_done = group.gather(dmiddle.astype(half))
    ffn, _ = group.scatter(lambda a: product_nt(a, w_down), hidden, done=(cot_done,))
    mixed = middle + ffn
    dheads = product(attn_cot, w_out)
    g_out = ring.scatter(product_tn(attn_cot, heads)).T
    dqkv, dcols = core_bwd(*core, dheads, att, lse, SEQ_LEN, turn)
    dnormed1, parts = group.scatter(lambda a: product_nt(a, w_in), dqkv)
    g_in = ring.scatter(product_tn(wide_one, dqkv), (width // 2,))
    dx_norm, gain_one = norm_back(x, rms1, gains[0], dnormed1)
    tokens_grad = dmiddle + dx_norm
    if group.pair:
        rows = wide_one.shape[0] // 2
        gain_one = sum(jnp.sum(part.astype(jnp.float32) * wide_one[n * rows:(n + 1) * rows], 0)
                       for n, part in enumerate(parts)) / gains[0]
        grad_gains, grad_persist = ring.total(jnp.stack([gain_one, gain_two]), dcols)
        grad_gains = grad_gains + group.other(grad_gains)
        across = group.other(grad_persist)
        grad_persist = jnp.where(place_at == 0, jnp.concatenate([grad_persist, across], 1),
                                 jnp.concatenate([across, grad_persist], 1))
    else:
        persist_part = lax.dynamic_update_slice_in_dim(jnp.zeros_like(persist), dcols, start, 1)
        grad_gains, grad_persist = lax.psum((jnp.stack([gain_one, gain_two]), persist_part), ("dp", "tensor"))
    return (
        mixed,
        tokens_grad,
        *advance(inward, momentum_inward, average_inward, g_in),
        *advance(outward, momentum_outward, average_outward, g_out),
        *advance(gateup, momentum_gateup, average_gateup, g_gu),
        *advance(downward, momentum_downward, average_downward, g_down),
        *advance(gains, momentum_gains, average_gains, grad_gains),
        *advance(persist, momentum_persist, average_persist, grad_persist, LEARN_PERSIST),
    )


def solution(mesh):
    rows, by_in, by_out = P(("dp", "tensor"), None), P("dp", "tensor"), P("tensor", "dp")
    by_gu = P(None, "dp", "tensor")
    weights = (by_in, by_out, by_gu, by_out, P(), P())
    outs = [rows, rows]
    for spec in weights:
        outs += [spec] * 5
    group = Group(mesh.shape["tensor"])
    return jax.shard_map(
        functools.partial(shards, group, Ring(mesh.shape["dp"], group.pair)),
        mesh=mesh,
        in_specs=(rows, P("dp"), by_out, by_out, rows) + weights * 3,
        out_specs=tuple(outs),
        check_vma=False,
    )
```
